32 devices in a mesh: dp: 8 (over z, x), expert: 4 (over y, core).
Axes of the slice: x: 2, y: 2, z: 4, core: 2. Of those that a mesh axis runs over, the one named last changes fastest.
Arguments:
- tokens: bfloat16 [4096, 1024], P(('dp', 'expert')), may hold values from -24 to 24
- cotangent: bfloat16 [4096, 1024], P(('dp', 'expert')), may hold values from -6 to 6
- prefix: int32 [8], P('dp'), may hold values from 51 to 256
- expert_choice: int32 [4096, 1], P(('dp', 'expert')), may hold values from 0 to 3; in each aligned block of 128 rows (0 to 127, 128 to 255, ...) at most 64 rows name the same one
- norm1_gain: bfloat16 [1024], P(('dp', 'expert')), may hold values from 0.099609375 to 1.8984375
- w_qkv: bfloat16 [1024, 3072], P(('dp', 'expert')), may hold values from -0.1875 to 0.1875
- w_out: bfloat16 [1024, 1024], P(('dp', 'expert')), may hold values from -1.5 to 1.5
- norm2_gain: bfloat16 [1024], P(('dp', 'expert')), may hold values from 0.099609375 to 1.8984375
- w_up: bfloat16 [1024, 4096], P(('dp', 'expert')), may hold values from -0.1875 to 0.1875
- w_down: bfloat16 [4096, 1024], P(('dp', 'expert')), may hold values from -0.09375 to 0.09375
- w_router: bfloat16 [1024, 4], P(('dp', 'expert')), may hold values from -0.125 to 0.125
- w_mix: bfloat16 [1024, 2], P(('dp', 'expert')), may hold values from -0.1875 to 0.1875
- expert_up: bfloat16 [4096, 4, 1024], P('dp', 'expert'), may hold values from -0.1875 to 0.1875
- expert_down: bfloat16 [4096, 4, 1024], P('dp', 'expert'), may hold values from -0.375 to 0.375
Outputs:
- output: float32 [4096, 1024], P(('dp', 'expert'))
- grad_tokens: float32 [4096, 1024], P(('dp', 'expert'))
- grad_norm1_gain: float32 [1024], P(('dp', 'expert'))
- grad_w_qkv: float32 [1024, 3072], P(('dp', 'expert'))
- grad_w_out: float32 [1024, 1024], P(('dp', 'expert'))
- grad_norm2_gain: float32 [1024], P(('dp', 'expert'))
- grad_w_up: float32 [1024, 4096], P(('dp', 'expert'))
- grad_w_down: float32 [4096, 1024], P(('dp', 'expert'))
- grad_w_router: float32 [1024, 4], P(('dp', 'expert'))
- grad_w_mix: float32 [1024, 2], P(('dp', 'expert'))
- grad_expert_up: float32 [4096, 4, 1024], P('dp', 'expert')
- grad_expert_down: float32 [4096, 4, 1024], P('dp', 'expert')
- rms_mid: float32 [], replicated
- rms_attn: float32 [], replicated
- rms_ffn: float32 [], replicated
- rms_out: float32 [], replicated
The draws below stay inside these ranges and needn't reach their ends.
Inputs may be any that keep to these rules, and one draw needn't show every extreme that they name: `expert_choice`: among the 128 rows of one device no expert is chosen more than 64 times.
All inputs are finite; a program needn't handle non-finite values.
Results may differ from the reference program's by a relative error of at most 0.033.
Values may be sent and summed in bfloat16 or wider, within the bound.
A program may use at most 192 MiB of HBM per device.

```python
import math
import jax
import jax.numpy as jnp
import numpy as np
from jax import lax

D = 1024
HEADS = 16
HEAD = 64
FF = 4096
TOK_DEV = 128
EXPERTS = 4
CAP = 64
SEQ = 512
SEQS = 8
TOKENS = 4096
N_EXPERT = 4


def draw_tokens(key, part):
    key_base = jax.random.fold_in(key, 11)
    key_cols = jax.random.fold_in(key, 12)
    token_ramp = jnp.arange(TOKENS, dtype=jnp.float32) / TOKENS
    col_scale = jnp.exp(jax.random.uniform(key_cols, (D,), jnp.float32, math.log(0.3), math.log(3.0)))
    base_draw = jnp.clip(jax.random.normal(key_base, (TOKENS, D), jnp.float32), -4.0, 4.0)
    row_scale = 0.6 * jnp.exp(token_ramp * math.log(3.0))
    drawn = row_scale[:, None] * col_scale[None, :] * base_draw
    return drawn.astype(jnp.bfloat16)


def touch_ends(array, rng, smallest, high):
    longest = array.shape.index(max(array.shape))
    spots = []
    for shift in (0, 1):
        where = [jax.random.randint(jax.random.fold_in(rng, axis), (), 0, length) for axis, length in enumerate(array.shape)]
        where[longest] = (where[longest] + shift) % array.shape[longest]
        spots.append(tuple(where))
    return array.at[spots[0]].set(smallest).at[spots[1]].set(high)


def steps_of(key, extent, split, least, high):
    factor_of = 1.0
    for position, blocks in split:
        draws = jax.random.uniform(jax.random.fold_in(jax.random.fold_in(key, 6), position), (blocks,), jnp.float32, least / len(split), high / len(split))
        factor_of = factor_of * jnp.repeat(jnp.exp(draws), extent[position] // blocks).reshape((-1,) + (1,) * (len(extent) - 1 - position))
    return factor_of


def assign_block(key, own, number, rows, count, top, most, slope):
    order = jax.random.permutation(key, count)
    heavy_load, usual = load_shares(count, rows * top, most, slope, True), load_shares(count, rows * top, most, slope, False)
    places = jnp.arange(count)

    def named(sizes, turn):
        used = int((sizes > 0).sum())
        fixed = max(1, used // 4)
        moved = fixed + (places - fixed + turn * (used - fixed)) % max(1, count - fixed)
        return jnp.zeros((count,), jnp.int32).at[order[jnp.where(places < fixed, places, moved)]].set(jnp.asarray(sizes, jnp.int32))

    sizes = jnp.where(number % 4 == 0, named(heavy_load, number // 4), named(usual, number - number // 4 - 1))
    mixed = jax.random.permutation(jax.random.fold_in(own, 3), count)
    donor, receiver = mixed[0:count // 2 * 2:2], mixed[1:count // 2 * 2:2]
    margin = jnp.minimum(sizes[donor] - 1, most - sizes[receiver]) // 2
    margin = jnp.where((donor == order[0]) | (receiver == order[0]) | (sizes[receiver] == 0), 0, jnp.maximum(margin, 0))
    moved = jax.random.randint(jax.random.fold_in(own, 4), (count // 2,), 0, 1 << 20) % (margin + 1)
    sizes = sizes.at[donor].add(-moved).at[receiver].add(moved)
    members = jnp.searchsorted(jnp.cumsum(sizes), jnp.arange(rows * top), side="right").astype(jnp.int32)
    listing = members.reshape(top, rows).T
    listing = listing[jax.random.permutation(jax.random.fold_in(own, 1), rows)]
    turn = jax.random.randint(jax.random.fold_in(own, 2), (rows, 1), 0, top)
    return jnp.take_along_axis(listing, (jnp.arange(top)[None, :] + turn) % top, axis=1)


def load_shares(number_of, total, reach, slope, full):
    loads = [(1 << 20) // math.isqrt(standing ** slope) + 1 for standing in range(1, number_of + 1)]
    largest = reach if full else min(reach, max(-(-total // number_of), total * loads[0] // sum(loads)))
    least = 1 if total - largest >= number_of - 1 else 0
    given, surplus = [largest] + [least] * (number_of - 1), total - largest - least * (number_of - 1)
    while surplus > 0:
        free = [i for i in range(1, number_of) if given[i] < largest] or [i for i in range(1, number_of) if given[i] < reach]
        pool, left = sum([loads[i] for i in free]), surplus
        for i in free:
            addition = min(reach - given[i], max(1, left * loads[i] // pool), surplus)
            given[i] = given[i] + addition
            surplus = surplus - addition
    return np.array(given)


def gaussian(own_key, shape, width, bound, shards=(), kind=jnp.bfloat16):
    loudness = steps_of(own_key, shape, shards, -0.22, 0.18) if shards else 1.0
    entries = jax.random.normal(own_key, shape, jnp.float32) * width * loudness
    return jnp.minimum(jnp.maximum(entries, -bound), bound).astype(kind)


def setup_inputs(seed: int = 0) -> dict:
    splits = jax.random.split(jax.random.key(seed), 15)
    tokens = draw_tokens(jax.random.fold_in(splits[14], 71), 0)
    cotangent = gaussian(splits[1], (TOKENS, D), 1.0, 6.0, ((0, 32),))
    prefix = touch_ends(jax.random.randint(splits[2], (SEQS,), SEQ // 10, SEQ // 2 + 1), jax.random.fold_in(splits[2], 1), SEQ // 10, (SEQ // 2 + 1) - 1).astype(jnp.int32)
    expert_choice_keys = jax.random.split(jax.random.fold_in(splits[3], 1), TOKENS // TOK_DEV)
    expert_choice_turns = jax.random.permutation(jax.random.fold_in(splits[3], 3), TOKENS // TOK_DEV)
    expert_choice = jax.vmap(lambda own, number: assign_block(jax.random.fold_in(splits[3], 2), own, number, TOK_DEV, EXPERTS, 1, CAP, 1))(expert_choice_keys, expert_choice_turns).reshape((TOKENS, 1))
    norm1_gain = jnp.clip(1.0 + 0.18 * jax.random.normal(splits[4], (D,), jnp.float32), 0.099609375, 1.8984375).astype(jnp.bfloat16)
    w_qkv = gaussian(splits[5], (D, 3 * D), D ** -0.5, 0.1875, ((0, 32),))
    w_out = gaussian(splits[6], (D, D), (D // 64) ** -0.5, 1.5, ((0, 32),))
    norm2_gain = jnp.clip(1.0 + 0.18 * jax.random.normal(splits[7], (D,), jnp.float32), 0.099609375, 1.8984375).astype(jnp.bfloat16)
    w_up = gaussian(splits[8], (D, FF), D ** -0.5, 0.1875, ((0, 32),))
    w_down = gaussian(splits[9], (FF, D), FF ** -0.5, 0.09375, ((0, 32),))
    w_router = gaussian(splits[10], (D, EXPERTS), (2 * D) ** -0.5, 0.125, ((0, 32),))
    w_mix = gaussian(splits[11], (D, 2), D ** -0.5, 0.1875, ((0, 32),))
    expert_up = gaussian(splits[12], (FF, EXPERTS, D), D ** -0.5, 0.1875, ((0, 8), (1, 4)))
    expert_down = gaussian(splits[13], (FF, EXPERTS, D), (FF // (EXPERTS * EXPERTS)) ** -0.5, 0.375, ((0, 8), (1, 4)))
    return {"tokens": tokens, "cotangent": cotangent, "prefix": prefix, "expert_choice": expert_choice, "norm1_gain": norm1_gain, "w_qkv": w_qkv, "w_out": w_out, "norm2_gain": norm2_gain, "w_up": w_up, "w_down": w_down, "w_router": w_router, "w_mix": w_mix, "expert_up": expert_up, "expert_down": expert_down}


@jax.custom_vjp
def low(v):
    return lax.optimization_barrier(v.astype(jnp.bfloat16)).astype(jnp.float32)

@jax.custom_vjp
def low_back(v):
    return v

def low_keep(v):
    return (low(v), None)

def low_pass(kept, grad):
    return (grad,)

def back_keep(v):
    return (v, None)

def back_low(kept, grad):
    return (low(grad),)
low.defvjp(low_keep, low_pass)
low_back.defvjp(back_keep, back_low)
HIGHEST = lax.Precision.HIGHEST
EPS = 1e-05
NEG_FILL = -1e+30

def both_round(values):
    return low(low_back(values))

def norm_rows(values, norm_gain):
    row_mean = lax.optimization_barrier(jnp.mean(values, axis=-1, keepdims=True))
    centered = values - row_mean
    variance = lax.optimization_barrier(jnp.mean(centered * centered, axis=-1, keepdims=True))
    return centered * lax.rsqrt(variance + EPS) * norm_gain

def gelu_tanh(values):
    return jax.nn.gelu(values, approximate=True)

def sequence_layer(params, seq_tokens, prefix_len, chosen):
    gain_one, w_qkv, w_out, gain_two, w_up, w_down, w_router, w_mix, expert_up, expert_down = params
    seq_len = seq_tokens.shape[0]
    normed = low(norm_rows(seq_tokens, gain_one))
    qkv_rows = both_round(jnp.dot(normed, w_qkv, precision=HIGHEST))
    queries = qkv_rows[:, :D].reshape(seq_len, HEADS, HEAD)
    key_heads = qkv_rows[:, D:2 * D].reshape(seq_len, HEADS, HEAD)
    value_heads = qkv_rows[:, 2 * D:].reshape(seq_len, HEADS, HEAD)
    positions = jnp.arange(seq_len, dtype=jnp.int32)
    visible = (positions[None, :] <= positions[:, None]) | (positions[None, :] < prefix_len)
    scores = low_back(jnp.einsum('qhd,khd->hqk', queries, key_heads, precision=HIGHEST) * HEAD ** (-0.5))
    scores = jnp.where(visible[None], scores, NEG_FILL)
    weights = low(jax.nn.softmax(scores, axis=-1))
    attended = both_round(jnp.einsum('hqk,khd->qhd', weights, value_heads, precision=HIGHEST).reshape(seq_len, D))
    attn_out = low_back(jnp.dot(attended, w_out, precision=HIGHEST))
    middle = seq_tokens + attn_out
    hidden = low(norm_rows(middle, gain_two))
    router_probs = jax.nn.softmax(jnp.dot(hidden, w_router, precision=HIGHEST), axis=-1)
    onehot = (jnp.arange(EXPERTS, dtype=jnp.int32)[None, :] == chosen[:, None]).astype(jnp.float32)
    gate_prob = lax.optimization_barrier(jnp.sum(router_probs * onehot, axis=-1))
    mix_coef = jax.nn.softmax(jnp.dot(hidden, w_mix, precision=HIGHEST), axis=-1)
    dense_act = low(gelu_tanh(low_back(jnp.dot(hidden, w_up, precision=HIGHEST))))
    dense_out = low_back(jnp.dot(dense_act, w_down, precision=HIGHEST))
    onehot_int = (jnp.arange(EXPERTS, dtype=jnp.int32)[None, :] == chosen[:, None]).astype(jnp.int32)
    counts = onehot_int.reshape(N_EXPERT, TOK_DEV, EXPERTS)
    before = (jnp.cumsum(counts, axis=1) - counts).reshape(seq_len, EXPERTS)
    slot_rank = lax.optimization_barrier(jnp.sum(before * onehot_int, axis=-1)).astype(jnp.int32)
    device_block = (positions // TOK_DEV).astype(jnp.int32)
    slot_index = (chosen * (N_EXPERT * CAP) + device_block * CAP + slot_rank).astype(jnp.int32)
    buffer = jnp.zeros((EXPERTS * N_EXPERT * CAP, D), jnp.float32).at[slot_index].set(hidden)
    buffer = low_back(buffer).reshape(EXPERTS, N_EXPERT * CAP, D)
    expert_pre = low_back(jnp.einsum('ecd,fed->ecf', buffer, expert_up, precision=HIGHEST))
    expert_act = low(gelu_tanh(expert_pre))
    expert_out = both_round(jnp.einsum('ecf,fed->ecd', expert_act, expert_down, precision=HIGHEST))
    expert_rows = expert_out.reshape(EXPERTS * N_EXPERT * CAP, D)[slot_index]
    branch = mix_coef[:, 0:1] * dense_out + (mix_coef[:, 1] * gate_prob)[:, None] * expert_rows
    result = middle + branch
    return (result, (jnp.sum(middle * middle), jnp.sum(attn_out * attn_out), jnp.sum(branch * branch), jnp.sum(result * result)))

def reference(tokens, cotangent, prefix, expert_choice, norm1_gain, w_qkv, w_out, norm2_gain, w_up, w_down, w_router, w_mix, expert_up, expert_down):
    params = tuple((weight.astype(jnp.float32) for weight in (norm1_gain, w_qkv, w_out, norm2_gain, w_up, w_down, w_router, w_mix, expert_up, expert_down)))
    seq_tokens = tokens.astype(jnp.float32).reshape(SEQS, SEQ, D)
    chosen = expert_choice[:, 0].astype(jnp.int32).reshape(SEQS, SEQ)
    layer_step = jax.checkpoint(sequence_layer)

    def forward(weights, inputs):

        def scan_step(carried, seq_item):
            result, squares = layer_step(weights, seq_item[0], seq_item[1], seq_item[2])
            return (carried, (result, squares))
        unused, (results, squares) = lax.scan(scan_step, jnp.zeros((), jnp.float32), (inputs, prefix, chosen))
        return (results, squares)
    results, pullback, squares = jax.vjp(forward, params, seq_tokens, has_aux=True)
    grad_params, grad_inputs = pullback(cotangent.astype(jnp.float32).reshape(SEQS, SEQ, D))
    entry_count = TOKENS * D
    rms_mid = jnp.sqrt(jnp.sum(squares[0]) / entry_count + 1e-06)
    rms_attn = jnp.sqrt(jnp.sum(squares[1]) / entry_count + 1e-06)
    rms_ffn = jnp.sqrt(jnp.sum(squares[2]) / entry_count + 1e-06)
    rms_out = jnp.sqrt(jnp.sum(squares[3]) / entry_count + 1e-06)
    return (results.reshape(TOKENS, D), grad_inputs.reshape(TOKENS, D), grad_params[0], grad_params[1], grad_params[2], grad_params[3], grad_params[4], grad_params[5], grad_params[6], grad_params[7], grad_params[8], grad_params[9], rms_mid, rms_attn, rms_ffn, rms_out)
```

```python
import jax
import jax.numpy as jnp
from jax import lax
from jax.sharding import PartitionSpec as P

HEAD = 64


EPS = 1e-05
NEG_FILL = -1e30
HIGHEST = lax.Precision.HIGHEST
ROWS_AXIS = (((0,), (0,)), ((), ()))
COLS_AXIS = (((1,), (1,)), ((), ()))


def layer_norm(values, norm_gain):
    row_mean = jnp.mean(values, axis=-1, keepdims=True)
    centered = values - row_mean
    inverse = lax.rsqrt(jnp.mean(centered * centered, axis=-1, keepdims=True) + EPS)
    normed = centered * inverse
    return (normed * norm_gain, normed, inverse)


def norm_back(grad_out, normed, inverse, norm_gain):
    scaled = grad_out * norm_gain
    mean_one = jnp.mean(scaled, axis=-1, keepdims=True)
    mean_two = jnp.mean(scaled * normed, axis=-1, keepdims=True)
    return (inverse * (scaled - mean_one - normed * mean_two), jnp.sum(grad_out * normed, axis=0))


def gelu_tanh(values):
    return jax.nn.gelu(values, approximate=True)


def gelu_back(pre_act, grad_act):
    return jax.vjp(gelu_tanh, pre_act)[1](grad_act)[0]


def softmax_rows(logits):
    shifted = logits - jnp.max(logits, axis=-1, keepdims=True)
    weights = jnp.exp(shifted)
    return weights / jnp.sum(weights, axis=-1, keepdims=True)


def contract_rows(left_side, right_side):
    return lax.dot_general(left_side, right_side, ROWS_AXIS, preferred_element_type=jnp.float32)


def contract_cols(left_side, right_side):
    return lax.dot_general(left_side, right_side, COLS_AXIS, preferred_element_type=jnp.float32)


def precise_rows(left_side, right_side):
    return lax.dot_general(
        left_side, right_side, ROWS_AXIS, precision=HIGHEST, preferred_element_type=jnp.float32
    )


def precise_cols(left_side, right_side):
    return lax.dot_general(
        left_side, right_side, COLS_AXIS, precision=HIGHEST, preferred_element_type=jnp.float32
    )


def per_device(
    tokens,
    cotangent,
    prefix,
    expert_choice,
    norm1_gain,
    w_qkv,
    w_out,
    norm2_gain,
    w_up,
    w_down,
    w_router,
    w_mix,
    expert_up,
    expert_down,
):
    local_rows, model_width = tokens.shape
    experts = lax.axis_size("expert")
    replicas = lax.axis_size("dp")
    capacity = 2 * local_rows // experts
    cut_width = model_width // experts
    head_count = cut_width // HEAD
    ff_cut = w_up.shape[1] // experts
    row_share = w_qkv.shape[0]
    ff_share = w_down.shape[0]
    stride = replicas // experts
    my_block = lax.axis_index("dp") * experts + lax.axis_index("expert")
    score_scale = HEAD ** (-0.5)

    ff_own = replicas * ff_share

    def spread(rows_low):
        return lax.all_gather(rows_low, "expert", axis=0, tiled=True)

    def fold(partial_sums):
        return lax.psum_scatter(
            partial_sums.astype(jnp.bfloat16), "expert", scatter_dimension=0, tiled=True
        ).astype(jnp.float32)

    def swap(blocks):
        return lax.all_to_all(blocks, "expert", split_axis=0, concat_axis=0, tiled=True)

    def gather_dp(rows):
        return lax.all_gather(rows, "dp", axis=0, tiled=True)

    def scatter_dp(rows):
        return lax.psum_scatter(
            rows.astype(jnp.bfloat16), "dp", scatter_dimension=0, tiled=True
        )

    small = lax.all_gather(
        jnp.concatenate([norm1_gain[:, None], norm2_gain[:, None], w_router, w_mix], axis=1),
        ("dp", "expert"),
        axis=0,
        tiled=True,
    )
    gain_one = small[:, 0].astype(jnp.float32)
    gain_two = small[:, 1].astype(jnp.float32)
    router_w = small[:, 2 : 2 + experts]
    mix_w = small[:, 2 + experts :]

    qkv_out = jnp.moveaxis(w_qkv.reshape(row_share, 3, experts, cut_width), 2, 0)
    qkv_w = gather_dp(swap(qkv_out).reshape(experts * row_share, 3 * cut_width))
    out_rows = gather_dp(w_out)
    out_in = swap(out_rows.reshape(experts, stride * row_share, model_width))
    out_w = jnp.transpose(
        out_in.reshape(experts, stride, row_share, model_width), (1, 0, 2, 3)
    ).reshape(cut_width, model_width)
    up_out = jnp.moveaxis(w_up.reshape(row_share, replicas, experts, ff_share), 2, 0)
    up_w = gather_dp(swap(up_out).reshape(experts * row_share, ff_own))
    down_w = gather_dp(w_down)
    expert_in_w = expert_up[:, 0, :]
    expert_out_w = expert_down[:, 0, :]

    inputs = tokens.astype(jnp.float32)
    scaled_one, normed_one, inverse_one = layer_norm(inputs, gain_one)
    normed_all = spread(scaled_one.astype(jnp.bfloat16))
    seq_len = normed_all.shape[0]
    qkv_cut = jnp.dot(normed_all, qkv_w, preferred_element_type=jnp.float32).astype(jnp.bfloat16)
    queries = qkv_cut[:, :cut_width].reshape(seq_len, head_count, HEAD)
    keys = qkv_cut[:, cut_width : 2 * cut_width].reshape(seq_len, head_count, HEAD)
    values = qkv_cut[:, 2 * cut_width :].reshape(seq_len, head_count, HEAD)
    position = jnp.arange(seq_len, dtype=jnp.int32)
    visible = (position[None, :] <= position[:, None]) | (position[None, :] < prefix[0])
    masked = jnp.where(
        visible[None],
        jnp.einsum("qhd,khd->hqk", queries, keys, preferred_element_type=jnp.float32)
        * score_scale,
        NEG_FILL,
    )
    row_max = jnp.max(masked, axis=-1, keepdims=True)
    expd = jnp.exp(masked - row_max)
    probs = expd / jnp.sum(expd, axis=-1, keepdims=True)
    probs_low = probs.astype(jnp.bfloat16)
    attended_cut = (
        jnp.einsum("hqk,khd->qhd", probs_low, values, preferred_element_type=jnp.float32)
        .reshape(seq_len, cut_width)
        .astype(jnp.bfloat16)
    )
    attn_out = fold(jnp.dot(attended_cut, out_w, preferred_element_type=jnp.float32))
    middle = inputs + attn_out
    scaled_two, normed_two, inverse_two = layer_norm(middle, gain_two)
    hidden_low = scaled_two.astype(jnp.bfloat16)
    router_probs = softmax_rows(jnp.dot(hidden_low, router_w, preferred_element_type=jnp.float32))
    chosen = expert_choice[:, 0]
    onehot_int = (jnp.arange(experts, dtype=jnp.int32)[None, :] == chosen[:, None]).astype(
        jnp.int32
    )
    onehot = onehot_int.astype(jnp.float32)
    gate_prob = jnp.sum(router_probs * onehot, axis=-1)
    mix_coef = softmax_rows(jnp.dot(hidden_low, mix_w, preferred_element_type=jnp.float32))
    coef_dense = mix_coef[:, 0:1]
    coef_expert = (mix_coef[:, 1] * gate_prob)[:, None]
    grad_out = cotangent.astype(jnp.float32)
    grad_dense = (grad_out * coef_dense).astype(jnp.bfloat16)
    grad_expert = (grad_out * coef_expert).astype(jnp.bfloat16)

    row_id = jnp.arange(local_rows, dtype=jnp.int32)
    before = (row_id[:, None] > row_id[None, :]).astype(jnp.bfloat16)
    earlier = jnp.dot(before, onehot.astype(jnp.bfloat16), preferred_element_type=jnp.float32)
    slot_rank = jnp.sum(earlier * onehot, axis=-1).astype(jnp.int32)
    slot_index = chosen * capacity + slot_rank
    slot_rows = experts * capacity
    picks = (slot_index[:, None] == jnp.arange(slot_rows, dtype=jnp.int32)[None, :]).astype(
        jnp.bfloat16
    )
    send_rows = contract_rows(picks, jnp.concatenate([hidden_low, grad_expert], axis=1)).astype(
        jnp.bfloat16
    )
    received = swap(send_rows.reshape(experts, capacity, 2 * model_width))
    routed = gather_dp(received.reshape(slot_rows, 2 * model_width))
    routed_in = routed[:, :model_width]
    routed_grad = routed[:, model_width:]
    dense_rows = spread(jnp.concatenate([hidden_low, grad_dense], axis=1))
    hidden_all = dense_rows[:, :model_width]
    grad_dense_all = dense_rows[:, model_width:]

    dense_pre = jnp.dot(hidden_all, up_w, preferred_element_type=jnp.float32)
    dense_act = gelu_tanh(dense_pre).astype(jnp.bfloat16)
    grad_act_d = contract_cols(grad_dense_all, down_w)
    grad_pre_d = gelu_back(dense_pre, grad_act_d).astype(jnp.bfloat16)
    dense_sums = jnp.concatenate(
        [
            jnp.dot(dense_act, down_w, preferred_element_type=jnp.float32).astype(jnp.bfloat16),
            contract_cols(grad_pre_d, up_w).astype(jnp.bfloat16),
        ],
        axis=1,
    )
    dense_back = fold(dense_sums)
    dense_out = dense_back[:, :model_width]
    grad_w_down_cut = contract_rows(dense_act, grad_dense_all)
    grad_w_up_cut = contract_rows(hidden_all, grad_pre_d)

    pre_act = contract_cols(routed_in, expert_in_w)
    act_low = gelu_tanh(pre_act).astype(jnp.bfloat16)
    grad_act_e = contract_cols(routed_grad, expert_out_w)
    grad_pre_e = gelu_back(pre_act, grad_act_e).astype(jnp.bfloat16)
    expert_sums = jnp.concatenate(
        [
            jnp.dot(act_low, expert_out_w, preferred_element_type=jnp.float32).astype(
                jnp.bfloat16
            ),
            jnp.dot(grad_pre_e, expert_in_w, preferred_element_type=jnp.float32).astype(
                jnp.bfloat16
            ),
        ],
        axis=1,
    )
    grad_expert_up = contract_rows(grad_pre_e, routed_in)
    grad_expert_down = contract_rows(act_low, routed_grad)
    expert_back = swap(scatter_dp(expert_sums).reshape(experts, capacity, 2 * model_width))
    expert_rows_all = jnp.dot(
        picks, expert_back.reshape(slot_rows, 2 * model_width), preferred_element_type=jnp.float32
    )
    expert_rows = expert_rows_all[:, :model_width]

    ffn_out = coef_dense * dense_out + coef_expert * expert_rows
    result = middle + ffn_out
    square_stats = jnp.stack(
        [
            jnp.sum(middle * middle),
            jnp.sum(attn_out * attn_out),
            jnp.sum(ffn_out * ffn_out),
            jnp.sum(result * result),
        ]
    )
    dense_dot = jnp.sum(grad_out * dense_out, axis=-1)
    expert_dot = jnp.sum(grad_out * expert_rows, axis=-1)
    coef_grad = jnp.stack([dense_dot, expert_dot * gate_prob], axis=-1)
    grad_mix = mix_coef * (coef_grad - jnp.sum(mix_coef * coef_grad, axis=-1, keepdims=True))
    gate_grad = expert_dot * mix_coef[:, 1]
    grad_router = (gate_grad * gate_prob)[:, None] * (onehot - router_probs)

    hidden_wide = hidden_low.astype(jnp.float32)
    grad_hidden = dense_back[:, model_width:] + expert_rows_all[:, model_width:]
    grad_hidden = (
        grad_hidden
        + precise_cols(grad_router, router_w.astype(jnp.float32))
        + precise_cols(grad_mix, mix_w.astype(jnp.float32))
    )
    grad_w_router = precise_rows(grad_router, hidden_wide)
    grad_w_mix = precise_rows(grad_mix, hidden_wide)
    grad_mid_norm, grad_gain_two = norm_back(grad_hidden, normed_two, inverse_two, gain_two)
    grad_middle = grad_out + grad_mid_norm
    grad_attn_all = spread(grad_middle.astype(jnp.bfloat16))
    grad_w_out_cut = contract_rows(attended_cut, grad_attn_all)
    grad_att_cut = (
        contract_cols(grad_attn_all, out_w)
        .astype(jnp.bfloat16)
        .reshape(seq_len, head_count, HEAD)
    )

    grad_probs = jnp.einsum(
        "qhd,khd->hqk", grad_att_cut, values, preferred_element_type=jnp.float32
    )
    row_delta = jnp.sum(probs * grad_probs, axis=-1, keepdims=True)
    grad_scores = (probs * (grad_probs - row_delta)).astype(jnp.bfloat16)
    grad_query = (
        jnp.einsum("hqk,khd->qhd", grad_scores, keys, preferred_element_type=jnp.float32)
        * score_scale
    )
    grad_key = (
        jnp.einsum("hqk,qhd->khd", grad_scores, queries, preferred_element_type=jnp.float32)
        * score_scale
    )
    grad_value = jnp.einsum(
        "hqk,qhd->khd", probs_low, grad_att_cut, preferred_element_type=jnp.float32
    )
    grad_qkv_cut = jnp.concatenate(
        [
            grad_query.reshape(seq_len, cut_width),
            grad_key.reshape(seq_len, cut_width),
            grad_value.reshape(seq_len, cut_width),
        ],
        axis=1,
    ).astype(jnp.bfloat16)
    grad_w_qkv_cut = contract_rows(normed_all, grad_qkv_cut)
    grad_normed = fold(contract_cols(grad_qkv_cut, qkv_w))
    grad_in_norm, grad_gain_one = norm_back(grad_normed, normed_one, inverse_one, gain_one)
    grad_tokens = grad_middle + grad_in_norm

    up_sum = swap(
        scatter_dp(grad_w_up_cut).reshape(experts, row_share, replicas, ff_share)
    )
    grad_w_up = (
        jnp.transpose(up_sum, (1, 2, 0, 3)).reshape(row_share, experts * ff_own)
    ).astype(jnp.float32)
    grad_w_down = scatter_dp(grad_w_down_cut).astype(jnp.float32)
    out_send = jnp.transpose(
        grad_w_out_cut.astype(jnp.bfloat16).reshape(stride, experts, row_share, model_width),
        (1, 0, 2, 3),
    )
    grad_w_out = scatter_dp(swap(out_send).reshape(replicas * row_share, model_width)).astype(
        jnp.float32
    )
    qkv_sum = swap(scatter_dp(grad_w_qkv_cut).reshape(experts, row_share, 3, cut_width))
    grad_w_qkv = (
        jnp.transpose(qkv_sum, (1, 2, 0, 3)).reshape(row_share, 3 * model_width)
    ).astype(jnp.float32)

    totals = lax.psum(
        (
            jnp.concatenate(
                [grad_gain_one[None], grad_gain_two[None], grad_w_router, grad_w_mix], axis=0
            ),
            square_stats,
        ),
        ("dp", "expert"),
    )
    own = lax.dynamic_slice_in_dim(totals[0], my_block * row_share, row_share, 1)
    entry_count = local_rows * model_width * replicas * experts
    rms_values = jnp.sqrt(totals[1] / entry_count + 1e-06)
    return (
        result,
        grad_tokens,
        own[0],
        grad_w_qkv,
        grad_w_out,
        own[1],
        grad_w_up,
        grad_w_down,
        jnp.transpose(own[2 : 2 + experts]),
        jnp.transpose(own[2 + experts :]),
        grad_expert_up[:, None, :],
        grad_expert_down[:, None, :],
        rms_values[0],
        rms_values[1],
        rms_values[2],
        rms_values[3],
    )


def solution(mesh):
    return jax.shard_map(
        per_device,
        mesh=mesh,
        in_specs=(
            P(("dp", "expert"), None),
            P(("dp", "expert"), None),
            P("dp"),
            P(("dp", "expert"), None),
            P(("dp", "expert")),
            P(("dp", "expert"), None),
            P(("dp", "expert"), None),
            P(("dp", "expert")),
            P(("dp", "expert"), None),
            P(("dp", "expert"), None),
            P(("dp", "expert"), None),
            P(("dp", "expert"), None),
            P("dp", "expert", None),
            P("dp", "expert", None),
        ),
        out_specs=(
            P(("dp", "expert"), None),
            P(("dp", "expert"), None),
            P(("dp", "expert")),
            P(("dp", "expert"), None),
            P(("dp", "expert"), None),
            P(("dp", "expert")),
            P(("dp", "expert"), None),
            P(("dp", "expert"), None),
            P(("dp", "expert"), None),
            P(("dp", "expert"), None),
            P("dp", "expert", None),
            P("dp", "expert", None),
            P(),
            P(),
            P(),
            P(),
        ),
        check_vma=False,
    )
```

```python
import functools

import jax
import jax.numpy as jnp
from jax import lax
from jax.experimental import pallas as pl
from jax.experimental.pallas import tpu as pltpu
from jax.sharding import PartitionSpec as P

HEAD = 64


EPS = 1e-05
NEG_FILL = -1e30
HIGHEST = lax.Precision.HIGHEST
ROWS_AXIS = (((0,), (0,)), ((), ()))
COLS_AXIS = (((1,), (1,)), ((), ()))


def layer_norm(values, norm_gain):
    row_mean = jnp.mean(values, axis=-1, keepdims=True)
    centered = values - row_mean
    inverse = lax.rsqrt(jnp.mean(centered * centered, axis=-1, keepdims=True) + EPS)
    normed = centered * inverse
    return (normed * norm_gain, normed, inverse)


def norm_back(grad_out, normed, inverse, norm_gain):
    scaled = grad_out * norm_gain
    mean_one = jnp.mean(scaled, axis=-1, keepdims=True)
    mean_two = jnp.mean(scaled * normed, axis=-1, keepdims=True)
    return (inverse * (scaled - mean_one - normed * mean_two), jnp.sum(grad_out * normed, axis=0))


def gelu_tanh(values):
    return jax.nn.gelu(values, approximate=True)


def gelu_back(pre_act, grad_act):
    return jax.vjp(gelu_tanh, pre_act)[1](grad_act)[0]


def softmax_rows(logits):
    shifted = logits - jnp.max(logits, axis=-1, keepdims=True)
    weights = jnp.exp(shifted)
    return weights / jnp.sum(weights, axis=-1, keepdims=True)


def contract_rows(left_side, right_side):
    return lax.dot_general(left_side, right_side, ROWS_AXIS, preferred_element_type=jnp.float32)


def contract_cols(left_side, right_side):
    return lax.dot_general(left_side, right_side, COLS_AXIS, preferred_element_type=jnp.float32)


def precise_rows(left_side, right_side):
    return lax.dot_general(
        left_side, right_side, ROWS_AXIS, precision=HIGHEST, preferred_element_type=jnp.float32
    )


def precise_cols(left_side, right_side):
    return lax.dot_general(
        left_side, right_side, COLS_AXIS, precision=HIGHEST, preferred_element_type=jnp.float32
    )


MESH = pl.DeviceIdType.MESH
VMEM_SPEC = pl.BlockSpec(memory_space=pltpu.VMEM)
ANY_SPEC = pl.BlockSpec(memory_space=pl.ANY)
GRANT = 60 * 1024 * 1024


def comm_params(call_id):
    return pltpu.CompilerParams(
        collective_id=call_id, has_side_effects=True, vmem_limit_bytes=GRANT
    )


def remote(src, dst, send_sem, recv_sem, device):
    return pltpu.make_async_remote_copy(
        src_ref=src,
        dst_ref=dst,
        send_sem=send_sem,
        recv_sem=recv_sem,
        device_id=device,
        device_id_type=MESH,
    )


def exchange_kernel(axis, outer, inner, gathers, swaps, *refs):
    count = outer * inner
    total = gathers + swaps
    ins, outs = refs[:total], refs[total : 2 * total]
    send, recv, local, swap_send = refs[2 * total :]
    me = lax.axis_index(axis)
    row, col = me // inner, me % inner
    barrier = pltpu.get_barrier_semaphore()
    if swaps:
        for step in range(1, count):
            pl.semaphore_signal(
                barrier, inc=1, device_id={axis: (me + step) % count}, device_id_type=MESH
            )
        pl.semaphore_wait(barrier, count - 1)
    else:
        for has, peer in ways(row, col, outer, inner, me):

            @pl.when(has)
            def _(peer=peer):
                pl.semaphore_signal(barrier, inc=1, device_id={axis: peer}, device_id_type=MESH)

        pl.semaphore_wait(barrier, neighbours(row, col, outer, inner))

    def hop(item, index, src, way, peer):
        return remote(
            src,
            outs[item].at[index],
            send.at[item, way, index],
            recv.at[item, index],
            {axis: peer},
        )

    links = ways(row, col, outer, inner, me)
    started = []

    def start(item, index, src, way, extra):
        has, peer = links[way]
        cond = has if extra is None else jnp.logical_and(has, extra)

        @pl.when(cond)
        def _():
            hop(item, index, src, way, peer).start()

        started.append((item, index, src, way, cond))

    def arrived(item, index):
        hop(item, index, outs[item].at[index], 0, me).wait_recv()

    own = []
    for item in range(gathers):
        copy = pltpu.make_async_copy(ins[item], outs[item].at[me], local.at[item])
        for way in range(4):
            start(item, me, ins[item], way, None)
        copy.start()
        own.append(copy)
    for slot in range(swaps):
        item = gathers + slot
        for step in range(1, count):
            peer = (me + step) % count
            remote(
                ins[item].at[peer],
                outs[item].at[me],
                swap_send.at[slot, step],
                recv.at[item, me],
                {axis: peer},
            ).start()
        copy = pltpu.make_async_copy(ins[item].at[me], outs[item].at[me], local.at[item])
        copy.start()
        own.append(copy)
    for item in range(gathers):
        for far in range(1, outer):
            for sign, onward in ((-1, 0), (1, 1)):
                source = row + sign * far
                valid = jnp.logical_and(source >= 0, source < outer)
                index = jnp.clip(source, 0, outer - 1) * inner + col

                @pl.when(valid)
                def _(item=item, index=index):
                    arrived(item, index)

                for way in (onward, 2, 3):
                    start(item, index, outs[item].at[index], way, valid)
    for item in range(gathers):
        for source in range(outer):
            arrived(item, source * inner + 1 - col)
    for slot in range(swaps):
        item = gathers + slot
        for step in range(1, count):
            arrived(item, (me + step) % count)
    for copy in own:
        copy.wait()
    for item, index, src, way, cond in started:

        @pl.when(cond)
        def _(item=item, index=index, src=src, way=way):
            hop(item, index, src, way, me).wait_send()

    for slot in range(swaps):
        item = gathers + slot
        for step in range(1, count):
            remote(
                ins[item].at[(me + step) % count],
                outs[item].at[me],
                swap_send.at[slot, step],
                recv.at[item, me],
                {axis: me},
            ).wait_send()


def ways(row, col, outer, inner, me):
    count = outer * inner
    return (
        (row < outer - 1, jnp.minimum(me + inner, count - 1)),
        (row > 0, jnp.maximum(me - inner, 0)),
        (col < inner - 1, jnp.minimum(me + 1, count - 1)),
        (col > 0, jnp.maximum(me - 1, 0)),
    )


def neighbours(row, col, outer, inner):
    return (
        4
        - (row == 0).astype(jnp.int32)
        - (row == outer - 1).astype(jnp.int32)
        - (col == 0).astype(jnp.int32)
        - (col == inner - 1).astype(jnp.int32)
    )


def exchange(axis, outer, call_id, gathers=(), swaps=()):
    count = lax.axis_size(axis)
    inner = count // outer
    items = tuple(gathers) + tuple(swaps)
    shapes = [(count,) + item.shape for item in gathers] + [item.shape for item in swaps]
    outs = pl.pallas_call(
        functools.partial(exchange_kernel, axis, outer, inner, len(gathers), len(swaps)),
        out_shape=[
            jax.ShapeDtypeStruct(shape, item.dtype) for shape, item in zip(shapes, items)
        ],
        in_specs=[VMEM_SPEC] * len(items),
        out_specs=[ANY_SPEC] * len(items),
        scratch_shapes=[
            pltpu.SemaphoreType.DMA((max(1, len(gathers)), 4, count)),
            pltpu.SemaphoreType.DMA((len(items), count)),
            pltpu.SemaphoreType.DMA((len(items),)),
            pltpu.SemaphoreType.DMA((max(1, len(swaps)), count)),
        ],
        compiler_params=comm_params(call_id),
        name=f"exchange_{call_id}",
    )(*items)
    return outs


def add_rows(target, first, second, start, rows):
    step = 16

    def body(index, carry):
        where = pl.ds(pl.multiple_of(start + index * step, step), step)
        target[where, :] = (
            first[where, :].astype(jnp.float32) + second[where, :].astype(jnp.float32)
        ).astype(target.dtype)
        return carry

    lax.fori_loop(0, rows // step, body, 0)


def reduce_kernel(axis, outer, items, parts, *refs):
    inner = 2
    count = outer * inner
    ins, outs = refs[:items], refs[items : 2 * items]
    scratch = refs[2 * items :]
    near, held, above, below = (scratch[k * items : (k + 1) * items] for k in range(4))
    near_send, near_recv, far_send, up_recv, down_recv = scratch[4 * items :]
    me = lax.axis_index(axis)
    row, col = me // inner, me % inner
    partner = me + 1 - 2 * col
    links = ways(row, col, outer, inner, me)
    barrier = pltpu.get_barrier_semaphore()
    for has, peer in links:

        @pl.when(has)
        def _(peer=peer):
            pl.semaphore_signal(barrier, inc=1, device_id={axis: peer}, device_id_type=MESH)

    pl.semaphore_wait(barrier, neighbours(row, col, outer, inner))

    high = row >= (outer + 1) // 2
    mirrored = jnp.where(high, outer - 1 - row, row)

    def target_of(step):
        if step == outer - 1:
            return row
        guess = outer - 1 - step
        guess = jnp.where(guess <= mirrored, guess - 1, guess)
        return jnp.where(high, outer - 1 - guess, guess)

    def piece(item, part):
        rows = ins[item].shape[1] // parts
        return pl.ds(part * rows, rows), part * rows, rows

    def near_hop(item, part, goal):
        where = piece(item, part)[0]
        return remote(
            ins[item].at[goal * inner + 1 - col, where],
            near[item].at[goal, where],
            near_send.at[item, part, goal],
            near_recv.at[item, part, goal],
            {axis: partner},
        )

    def far_hop(item, part, goal, landing, sems, peer):
        where = piece(item, part)[0]
        return remote(
            held[item].at[goal, where],
            landing[item].at[goal, where],
            far_send.at[item, part, goal],
            sems.at[item, part, goal],
            {axis: peer},
        )

    for step in range(outer):
        goal = target_of(step)
        for item in range(items):
            for part in range(parts):
                near_hop(item, part, goal).start()
    for step in range(outer - 1):
        goal = target_of(step)
        going_up = goal > row
        going_down = goal < row
        for item in range(items):
            for part in range(parts):
                where, start, rows = piece(item, part)
                near_hop(item, part, goal).wait_recv()
                add_rows(
                    held[item].at[goal],
                    ins[item].at[goal * inner + col],
                    near[item].at[goal],
                    start,
                    rows,
                )

                @pl.when(jnp.logical_and(going_up, row > 0))
                def _():
                    far_hop(item, part, goal, above, up_recv, me).wait_recv()
                    add_rows(held[item].at[goal], held[item].at[goal], above[item].at[goal], start, rows)

                @pl.when(jnp.logical_and(going_down, row < outer - 1))
                def _():
                    far_hop(item, part, goal, below, down_recv, me).wait_recv()
                    add_rows(held[item].at[goal], held[item].at[goal], below[item].at[goal], start, rows)

                @pl.when(going_up)
                def _():
                    far_hop(item, part, goal, above, up_recv, links[0][1]).start()

                @pl.when(going_down)
                def _():
                    far_hop(item, part, goal, below, down_recv, links[1][1]).start()

    for item in range(items):
        for part in range(parts):
            where, start, rows = piece(item, part)
            near_hop(item, part, row).wait_recv()
            add_rows(outs[item], ins[item].at[me], near[item].at[row], start, rows)

            @pl.when(row > 0)
            def _():
                far_hop(item, part, row, above, up_recv, me).wait_recv()
                add_rows(outs[item], outs[item], above[item].at[row], start, rows)

            @pl.when(row < outer - 1)
            def _():
                far_hop(item, part, row, below, down_recv, me).wait_recv()
                add_rows(outs[item], outs[item], below[item].at[row], start, rows)

    for step in range(outer):
        goal = target_of(step)
        for item in range(items):
            for part in range(parts):
                near_hop(item, part, goal).wait_send()
                if step < outer - 1:
                    far_hop(item, part, goal, above, up_recv, me).wait_send()


def reduce_to_owner(axis, outer, call_id, items, parts, out_dtype):
    count = len(items)
    shapes = [item.shape for item in items]
    buffers = [pltpu.VMEM((outer,) + shape[1:], jnp.bfloat16) for shape in shapes]
    return pl.pallas_call(
        functools.partial(reduce_kernel, axis, outer, count, parts),
        out_shape=[jax.ShapeDtypeStruct(shape[1:], out_dtype) for shape in shapes],
        in_specs=[VMEM_SPEC] * count,
        out_specs=[VMEM_SPEC] * count,
        scratch_shapes=buffers * 4
        + [
            pltpu.SemaphoreType.DMA((count, parts, outer)),
            pltpu.SemaphoreType.DMA((count, parts, outer)),
            pltpu.SemaphoreType.DMA((count, parts, outer)),
            pltpu.SemaphoreType.DMA((count, parts, outer)),
            pltpu.SemaphoreType.DMA((count, parts, outer)),
        ],
        compiler_params=comm_params(call_id),
        name=f"reduce_{call_id}",
    )(*items)


def everyone_kernel(devices, group, summing, in_ref, out_ref, held, send, recv):
    me = lax.axis_index("dp") * group + lax.axis_index("expert")
    barrier = pltpu.get_barrier_semaphore()

    def place(step):
        peer = lax.rem(me + step, devices)
        return peer, {"dp": peer // group, "expert": lax.rem(peer, group)}

    def greet(step, carry):
        pl.semaphore_signal(barrier, inc=1, device_id=place(step)[1], device_id_type=MESH)
        return carry

    lax.fori_loop(1, devices, greet, 0)
    pl.semaphore_wait(barrier, devices - 1)

    def hop(step):
        peer, device = place(step)
        src = in_ref.at[peer] if summing else in_ref
        return remote(src, held.at[me], send.at[step], recv.at[me], device)

    def begin(step, carry):
        hop(step).start()
        return carry

    lax.fori_loop(1, devices, begin, 0)

    def finish(step, carry):
        peer = place(step)[0]
        src = in_ref.at[peer] if summing else in_ref
        remote(src, held.at[peer], send.at[step], recv.at[peer], place(step)[1]).wait()
        return carry

    lax.fori_loop(1, devices, finish, 0)
    held[me] = in_ref[me] if summing else in_ref[...]
    if summing:
        out_ref[...] = lax.fori_loop(
            1, devices, lambda index, total: total + held[index], held[0]
        )
    else:
        out_ref[...] = held[...]


def everyone(block, devices, group, call_id, summing):
    shape = block.shape[1:] if summing else block.shape
    return pl.pallas_call(
        functools.partial(everyone_kernel, devices, group, summing),
        out_shape=jax.ShapeDtypeStruct(shape if summing else (devices,) + shape, block.dtype),
        in_specs=[VMEM_SPEC],
        out_specs=VMEM_SPEC,
        scratch_shapes=[
            pltpu.VMEM((devices,) + shape, block.dtype),
            pltpu.SemaphoreType.DMA((devices,)),
            pltpu.SemaphoreType.DMA((devices,)),
        ],
        compiler_params=comm_params(call_id),
        name=f"everyone_{call_id}",
    )(block)


def per_device(
    tokens,
    cotangent,
    prefix,
    expert_choice,
    norm1_gain,
    w_qkv,
    w_out,
    norm2_gain,
    w_up,
    w_down,
    w_router,
    w_mix,
    expert_up,
    expert_down,
):
    local_rows, model_width = tokens.shape
    experts = lax.axis_size("expert")
    replicas = lax.axis_size("dp")
    capacity = 2 * local_rows // experts
    cut_width = model_width // experts
    head_count = cut_width // HEAD
    ff_cut = w_up.shape[1] // experts
    row_share = w_qkv.shape[0]
    ff_share = w_down.shape[0]
    stride = replicas // experts
    my_block = lax.axis_index("dp") * experts + lax.axis_index("expert")
    score_scale = HEAD ** (-0.5)

    ff_own = replicas * ff_share

    paired = experts == 4 and replicas == 8
    devices = replicas * experts

    def expert_exchange(call_id, gathers=(), swaps=()):
        if paired:
            outs = exchange("expert", 2, call_id, gathers, swaps)
            merged = [out.reshape((-1,) + out.shape[2:]) for out in outs[: len(gathers)]]
            return merged + list(outs[len(gathers) :])
        return [lax.all_gather(rows, "expert", axis=0, tiled=True) for rows in gathers] + [
            lax.all_to_all(blocks, "expert", split_axis=0, concat_axis=0, tiled=True)
            for blocks in swaps
        ]

    def gather_dp(call_id, arrays):
        if paired:
            outs = exchange("dp", 4, call_id, arrays)
            return [out.reshape((-1,) + out.shape[2:]) for out in outs]
        return [lax.all_gather(rows, "dp", axis=0, tiled=True) for rows in arrays]

    def scatter(axis, call_id, arrays, parts, out_dtype):
        lows = [rows.astype(jnp.bfloat16) for rows in arrays]
        if paired:
            count = lax.axis_size(axis)
            return reduce_to_owner(
                axis,
                count // 2,
                call_id,
                [rows.reshape(count, rows.shape[0] // count, rows.shape[1]) for rows in lows],
                parts,
                out_dtype,
            )
        return [
            lax.psum_scatter(rows, axis, scatter_dimension=0, tiled=True).astype(out_dtype)
            for rows in lows
        ]

    def fold(call_id, partial_sums):
        return scatter("expert", call_id, [partial_sums], 2, jnp.float32)[0]

    kinds = jnp.concatenate(
        [norm1_gain[None], norm2_gain[None], jnp.transpose(w_router), jnp.transpose(w_mix)], axis=0
    )
    kind_count = kinds.shape[0]
    if paired:
        padded = jnp.pad(kinds, ((0, 16 - kind_count), (0, 128 - row_share)))
        small = everyone(padded, devices, experts, 0, False)[:, :kind_count, :row_share]
        small = jnp.transpose(small, (1, 0, 2)).reshape(kind_count, model_width)
    else:
        small = lax.all_gather(kinds, ("dp", "expert"), axis=1, tiled=True)
    gain_one = small[0].astype(jnp.float32)
    gain_two = small[1].astype(jnp.float32)
    router_w = jnp.transpose(small[2 : 2 + experts])
    mix_w = jnp.transpose(small[2 + experts :])

    qkv_out = jnp.moveaxis(w_qkv.reshape(row_share, 3, experts, cut_width), 2, 0).reshape(
        experts, row_share, 3 * cut_width
    )
    up_out = jnp.moveaxis(w_up.reshape(row_share, replicas, experts, ff_share), 2, 0).reshape(
        experts, row_share, ff_own
    )
    qkv_in, up_in = expert_exchange(1, swaps=(qkv_out, up_out))
    qkv_w, out_rows, up_w, down_w = gather_dp(
        2,
        [
            qkv_in.reshape(experts * row_share, 3 * cut_width),
            w_out,
            up_in.reshape(experts * row_share, ff_own),
            w_down,
        ],
    )
    expert_in_w = expert_up[:, 0, :]
    expert_out_w = expert_down[:, 0, :]

    inputs = tokens.astype(jnp.float32)
    scaled_one, normed_one, inverse_one = layer_norm(inputs, gain_one)
    normed_all, out_in = expert_exchange(
        3,
        gathers=(scaled_one.astype(jnp.bfloat16),),
        swaps=(out_rows.reshape(experts, stride * row_share, model_width),),
    )
    out_w = jnp.transpose(
        out_in.reshape(experts, stride, row_share, model_width), (1, 0, 2, 3)
    ).reshape(cut_width, model_width)
    seq_len = normed_all.shape[0]
    qkv_cut = jnp.dot(normed_all, qkv_w, preferred_element_type=jnp.float32).astype(jnp.bfloat16)
    queries = qkv_cut[:, :cut_width].reshape(seq_len, head_count, HEAD)
    keys = qkv_cut[:, cut_width : 2 * cut_width].reshape(seq_len, head_count, HEAD)
    values = qkv_cut[:, 2 * cut_width :].reshape(seq_len, head_count, HEAD)
    position = jnp.arange(seq_len, dtype=jnp.int32)
    visible = (position[None, :] <= position[:, None]) | (position[None, :] < prefix[0])
    masked = jnp.where(
        visible[None],
        jnp.einsum("qhd,khd->hqk", queries, keys, preferred_element_type=jnp.float32)
        * score_scale,
        NEG_FILL,
    )
    row_max = jnp.max(masked, axis=-1, keepdims=True)
    expd = jnp.exp(masked - row_max)
    probs = expd / jnp.sum(expd, axis=-1, keepdims=True)
    probs_low = probs.astype(jnp.bfloat16)
    attended_cut = (
        jnp.einsum("hqk,khd->qhd", probs_low, values, preferred_element_type=jnp.float32)
        .reshape(seq_len, cut_width)
        .astype(jnp.bfloat16)
    )
    attn_out = fold(4, jnp.dot(attended_cut, out_w, preferred_element_type=jnp.float32))
    middle = inputs + attn_out
    scaled_two, normed_two, inverse_two = layer_norm(middle, gain_two)
    hidden_low = scaled_two.astype(jnp.bfloat16)
    router_probs = softmax_rows(jnp.dot(hidden_low, router_w, preferred_element_type=jnp.float32))
    chosen = expert_choice[:, 0]
    onehot_int = (jnp.arange(experts, dtype=jnp.int32)[None, :] == chosen[:, None]).astype(
        jnp.int32
    )
    onehot = onehot_int.astype(jnp.float32)
    gate_prob = jnp.sum(router_probs * onehot, axis=-1)
    mix_coef = softmax_rows(jnp.dot(hidden_low, mix_w, preferred_element_type=jnp.float32))
    coef_dense = mix_coef[:, 0:1]
    coef_expert = (mix_coef[:, 1] * gate_prob)[:, None]
    grad_out = cotangent.astype(jnp.float32)
    grad_dense = (grad_out * coef_dense).astype(jnp.bfloat16)
    grad_expert = (grad_out * coef_expert).astype(jnp.bfloat16)

    row_id = jnp.arange(local_rows, dtype=jnp.int32)
    before = (row_id[:, None] > row_id[None, :]).astype(jnp.bfloat16)
    earlier = jnp.dot(before, onehot.astype(jnp.bfloat16), preferred_element_type=jnp.float32)
    slot_rank = jnp.sum(earlier * onehot, axis=-1).astype(jnp.int32)
    slot_index = chosen * capacity + slot_rank
    slot_rows = experts * capacity
    picks = (slot_index[:, None] == jnp.arange(slot_rows, dtype=jnp.int32)[None, :]).astype(
        jnp.bfloat16
    )
    send_rows = contract_rows(picks, jnp.concatenate([hidden_low, grad_expert], axis=1)).astype(
        jnp.bfloat16
    )
    dense_rows, received = expert_exchange(
        5,
        gathers=(jnp.concatenate([hidden_low, grad_dense], axis=1),),
        swaps=(send_rows.reshape(experts, capacity, 2 * model_width),),
    )
    routed = gather_dp(6, [received.reshape(slot_rows, 2 * model_width)])[0]
    routed_in = routed[:, :model_width]
    routed_grad = routed[:, model_width:]
    hidden_all = dense_rows[:, :model_width]
    grad_dense_all = dense_rows[:, model_width:]

    dense_pre = jnp.dot(hidden_all, up_w, preferred_element_type=jnp.float32)
    dense_act = gelu_tanh(dense_pre).astype(jnp.bfloat16)
    grad_act_d = contract_cols(grad_dense_all, down_w)
    grad_pre_d = gelu_back(dense_pre, grad_act_d).astype(jnp.bfloat16)
    dense_sums = jnp.concatenate(
        [
            jnp.dot(dense_act, down_w, preferred_element_type=jnp.float32).astype(jnp.bfloat16),
            contract_cols(grad_pre_d, up_w).astype(jnp.bfloat16),
        ],
        axis=1,
    )
    dense_back = fold(7, dense_sums)
    dense_out = dense_back[:, :model_width]
    grad_w_down_cut = contract_rows(dense_act, grad_dense_all)
    grad_w_up_cut = contract_rows(hidden_all, grad_pre_d)

    pre_act = contract_cols(routed_in, expert_in_w)
    act_low = gelu_tanh(pre_act).astype(jnp.bfloat16)
    grad_act_e = contract_cols(routed_grad, expert_out_w)
    grad_pre_e = gelu_back(pre_act, grad_act_e).astype(jnp.bfloat16)
    expert_sums = jnp.concatenate(
        [
            jnp.dot(act_low, expert_out_w, preferred_element_type=jnp.float32).astype(
                jnp.bfloat16
            ),
            jnp.dot(grad_pre_e, expert_in_w, preferred_element_type=jnp.float32).astype(
                jnp.bfloat16
            ),
        ],
        axis=1,
    )
    grad_expert_up = contract_rows(grad_pre_e, routed_in)
    grad_expert_down = contract_rows(act_low, routed_grad)
    expert_sum = scatter("dp", 8, [expert_sums], 4, jnp.bfloat16)[0]
    expert_back = expert_exchange(
        9, swaps=(expert_sum.reshape(experts, capacity, 2 * model_width),)
    )[0]
    expert_rows_all = jnp.dot(
        picks, expert_back.reshape(slot_rows, 2 * model_width), preferred_element_type=jnp.float32
    )
    expert_rows = expert_rows_all[:, :model_width]

    ffn_out = coef_dense * dense_out + coef_expert * expert_rows
    result = middle + ffn_out
    square_stats = jnp.stack(
        [
            jnp.sum(middle * middle),
            jnp.sum(attn_out * attn_out),
            jnp.sum(ffn_out * ffn_out),
            jnp.sum(result * result),
        ]
    )
    dense_dot = jnp.sum(grad_out * dense_out, axis=-1)
    expert_dot = jnp.sum(grad_out * expert_rows, axis=-1)
    coef_grad = jnp.stack([dense_dot, expert_dot * gate_prob], axis=-1)
    grad_mix = mix_coef * (coef_grad - jnp.sum(mix_coef * coef_grad, axis=-1, keepdims=True))
    gate_grad = expert_dot * mix_coef[:, 1]
    grad_router = (gate_grad * gate_prob)[:, None] * (onehot - router_probs)

    hidden_wide = hidden_low.astype(jnp.float32)
    grad_hidden = dense_back[:, model_width:] + expert_rows_all[:, model_width:]
    grad_hidden = (
        grad_hidden
        + precise_cols(grad_router, router_w.astype(jnp.float32))
        + precise_cols(grad_mix, mix_w.astype(jnp.float32))
    )
    grad_w_router = precise_rows(grad_router, hidden_wide)
    grad_w_mix = precise_rows(grad_mix, hidden_wide)
    grad_mid_norm, grad_gain_two = norm_back(grad_hidden, normed_two, inverse_two, gain_two)
    grad_middle = grad_out + grad_mid_norm
    grad_attn_all = expert_exchange(10, gathers=(grad_middle.astype(jnp.bfloat16),))[0]
    grad_w_out_cut = contract_rows(attended_cut, grad_attn_all)
    grad_att_cut = (
        contract_cols(grad_attn_all, out_w)
        .astype(jnp.bfloat16)
        .reshape(seq_len, head_count, HEAD)
    )

    grad_probs = jnp.einsum(
        "qhd,khd->hqk", grad_att_cut, values, preferred_element_type=jnp.float32
    )
    row_delta = jnp.sum(probs * grad_probs, axis=-1, keepdims=True)
    grad_scores = (probs * (grad_probs - row_delta)).astype(jnp.bfloat16)
    grad_query = (
        jnp.einsum("hqk,khd->qhd", grad_scores, keys, preferred_element_type=jnp.float32)
        * score_scale
    )
    grad_key = (
        jnp.einsum("hqk,qhd->khd", grad_scores, queries, preferred_element_type=jnp.float32)
        * score_scale
    )
    grad_value = jnp.einsum(
        "hqk,qhd->khd", probs_low, grad_att_cut, preferred_element_type=jnp.float32
    )
    grad_qkv_cut = jnp.concatenate(
        [
            grad_query.reshape(seq_len, cut_width),
            grad_key.reshape(seq_len, cut_width),
            grad_value.reshape(seq_len, cut_width),
        ],
        axis=1,
    ).astype(jnp.bfloat16)
    grad_w_qkv_cut = contract_rows(normed_all, grad_qkv_cut)
    grad_normed = fold(11, contract_cols(grad_qkv_cut, qkv_w))
    grad_in_norm, grad_gain_one = norm_back(grad_normed, normed_one, inverse_one, gain_one)
    grad_tokens = grad_middle + grad_in_norm

    out_send = jnp.transpose(
        grad_w_out_cut.astype(jnp.bfloat16).reshape(stride, experts, row_share, model_width),
        (1, 0, 2, 3),
    ).reshape(experts, stride * row_share, model_width)
    out_mine = expert_exchange(12, swaps=(out_send,))[0].reshape(
        replicas * row_share, model_width
    )
    grad_w_down, up_sum, grad_w_out, qkv_sum = scatter(
        "dp", 13, [grad_w_down_cut, grad_w_up_cut, out_mine, grad_w_qkv_cut], 1, jnp.float32
    )
    up_back, qkv_back = expert_exchange(
        14,
        swaps=(
            up_sum.astype(jnp.bfloat16).reshape(experts, row_share, ff_own),
            qkv_sum.astype(jnp.bfloat16).reshape(experts, row_share, 3 * cut_width),
        ),
    )
    grad_w_up = (
        jnp.transpose(up_back.reshape(experts, row_share, replicas, ff_share), (1, 2, 0, 3))
        .reshape(row_share, experts * ff_own)
        .astype(jnp.float32)
    )
    grad_w_qkv = (
        jnp.transpose(qkv_back.reshape(experts, row_share, 3, cut_width), (1, 2, 0, 3))
        .reshape(row_share, 3 * model_width)
        .astype(jnp.float32)
    )

    kind_grads = jnp.concatenate(
        [grad_gain_one[None], grad_gain_two[None], grad_w_router, grad_w_mix], axis=0
    )
    if paired:
        slices = jnp.transpose(kind_grads.reshape(kind_count, devices, row_share), (1, 0, 2))
        slices = jnp.pad(slices, ((0, 0), (0, 0), (0, 128 - row_share)))
        stats = jnp.broadcast_to(
            jnp.pad(square_stats[None, None], ((0, 0), (0, 7), (0, 124))), (devices, 8, 128)
        )
        owned = everyone(
            jnp.concatenate([slices, stats], axis=1), devices, experts, 15, True
        )
        own = owned[:kind_count, :row_share]
        square_sums = owned[kind_count, :4]
    else:
        totals, square_sums = lax.psum((kind_grads, square_stats), ("dp", "expert"))
        own = lax.dynamic_slice_in_dim(totals, my_block * row_share, row_share, 1)
    entry_count = local_rows * model_width * replicas * experts
    rms_values = jnp.sqrt(square_sums / entry_count + 1e-06)
    return (
        result,
        grad_tokens,
        own[0],
        grad_w_qkv,
        grad_w_out,
        own[1],
        grad_w_up,
        grad_w_down,
        jnp.transpose(own[2 : 2 + experts]),
        jnp.transpose(own[2 + experts :]),
        grad_expert_up[:, None, :],
        grad_expert_down[:, None, :],
        rms_values[0],
        rms_values[1],
        rms_values[2],
        rms_values[3],
    )


def solution(mesh):
    return jax.shard_map(
        per_device,
        mesh=mesh,
        in_specs=(
            P(("dp", "expert"), None),
            P(("dp", "expert"), None),
            P("dp"),
            P(("dp", "expert"), None),
            P(("dp", "expert")),
            P(("dp", "expert"), None),
            P(("dp", "expert"), None),
            P(("dp", "expert")),
            P(("dp", "expert"), None),
            P(("dp", "expert"), None),
            P(("dp", "expert"), None),
            P(("dp", "expert"), None),
            P("dp", "expert", None),
            P("dp", "expert", None),
        ),
        out_specs=(
            P(("dp", "expert"), None),
            P(("dp", "expert"), None),
            P(("dp", "expert")),
            P(("dp", "expert"), None),
            P(("dp", "expert"), None),
            P(("dp", "expert")),
            P(("dp", "expert"), None),
            P(("dp", "expert"), None),
            P(("dp", "expert"), None),
            P(("dp", "expert"), None),
            P("dp", "expert", None),
            P("dp", "expert", None),
            P(),
            P(),
            P(),
            P(),
        ),
        check_vma=False,
    )
```
